128 devices in a mesh: lat: 4 (over x), ord: 16 (over y, z), batch: 2 (over core).
Axes of the slice: x: 4, y: 4, z: 4, core: 2. Of those that a mesh axis runs over, the one named last changes fastest.
Arguments:
- state_field: bfloat16 [512, 720, 1440], P(('batch', 'ord'), 'lat'), parts along dimension 0, may hold values from -6 to 6
- slot_order: int32 [512], replicated, may hold values from 0 to 511, each once
- legendre: bfloat16 [512, 720, 720], P(('lat', 'ord')), may hold values from -0.21875 to 0.21875
- degree_gain: float32 [720, 256], replicated, may hold values from 0.25 to 1.75
- mixing: bfloat16 [256, 256], replicated, may hold values from -0.375 to 0.375
Outputs:
- updated: bfloat16 [512, 720, 1440], P(('batch', 'ord'), 'lat'), parts along dimension 0
The draws below stay inside these ranges and needn't reach their ends.
There are 2 independent parts, one for each index of `batch`. The reference program is written for one: setup_inputs(seed, part) draws one part's arguments, and reference() takes and returns one part's arrays. A program takes and returns all parts, laid end to end along the dimension named above; an argument that names none is the same for every part. Nothing has to cross between parts.
Inputs may be any that keep to these rules, and one draw needn't show every extreme that they name: `slot_order`: each of 0 to 511 stands once.
All inputs are finite; a program needn't handle non-finite values.
Results may differ from the reference program's by a relative error of at most 0.0054.
Values may be sent and summed in bfloat16 or wider, within the bound.
A program may use at most 192 MiB of HBM per device.

```python
import math
import jax
import jax.numpy as jnp
from jax import lax

C = 256
NLAT = 720
NLON = 1440
L = 720
M = 512


def level_of(own_key, shape, pieces, low, high):
    def one(axis_at, shards_of):
        steps = jax.random.uniform(jax.random.fold_in(jax.random.fold_in(own_key, 6), axis_at), (shards_of,), jnp.float32, low / len(pieces), high / len(pieces))
        return jnp.repeat(jnp.exp(steps), shape[axis_at] // shards_of).reshape((-1,) + (1,) * (len(shape) - axis_at - 1))

    level = one(*pieces[0])
    for cut in pieces[1:]:
        level = level * one(*cut)
    return level


def normal_values(key, extent, scale, bound, split=(), kind=jnp.bfloat16):
    gain = level_of(key, extent, split, -0.22, 0.18) if split else 1.0
    drawn = jax.random.normal(key, extent, jnp.float32) * scale * gain
    return jnp.minimum(jnp.maximum(drawn, -bound), bound).astype(kind)


def setup_inputs(seed: int = 0, part: int = 0) -> dict:
    seeds = jax.random.split(jax.random.key(seed), 6)
    part_splits = jax.random.split(jax.random.fold_in(seeds[5], part), 6)
    return {
        "state_field": normal_values(part_splits[0], (C, NLAT, NLON), 1.0, 6.0, ((0, 16), (1, 4))),
        "slot_order": jax.random.permutation(seeds[1], M).astype(jnp.int32),
        "legendre": normal_values(seeds[2], (M, L, NLAT), NLAT ** -0.5, 0.21875, ((0, 64),)),
        "degree_gain": jnp.clip(jax.random.uniform(seeds[3], (L, C), jnp.float32, 0.25, 1.75), 0.25, 1.75),
        "mixing": normal_values(seeds[4], (C, C), C ** -0.5, 0.375),
    }


def tables(orders, lon_count):
    longitude = jnp.arange(lon_count, dtype=jnp.int32)
    phase = longitude[:, None] * orders[None, :].astype(jnp.int32) % lon_count
    angle = phase.astype(jnp.float32) * (2.0 * math.pi / lon_count)
    root = 1.0 / math.sqrt(lon_count)
    forward = jnp.concatenate([jnp.cos(angle) * root, -jnp.sin(angle) * root], axis=1).astype(jnp.bfloat16)
    weights = jnp.where(orders == 0, 1.0, 2.0).astype(jnp.float32) * root
    inverse = jnp.concatenate([jnp.cos(angle).T * weights[:, None], -jnp.sin(angle).T * weights[:, None]], axis=0).astype(jnp.bfloat16)
    return (forward, inverse)

def reference(state_field, slot_order, legendre, degree_gain, mixing):
    high = lax.Precision.HIGHEST
    forward, inverse = tables(slot_order, NLON)
    flat = state_field.reshape(C * NLAT, NLON).astype(jnp.float32)
    fourier = jnp.dot(flat, forward.astype(jnp.float32), precision=high, preferred_element_type=jnp.float32).astype(jnp.bfloat16)
    fourier = fourier.reshape(C, NLAT, 2, M).transpose(3, 1, 2, 0).reshape(M, NLAT, 2 * C)
    padded_gain = jnp.concatenate([degree_gain, jnp.zeros((L, C), jnp.float32)], axis=0)
    mix_wide = mixing.astype(jnp.float32)

    def per_slot(item):
        slot_table, coeffs, order = item
        table_wide = slot_table.astype(jnp.float32)
        spec = jnp.dot(table_wide, coeffs.astype(jnp.float32), precision=high, preferred_element_type=jnp.float32)
        gain_rows = lax.dynamic_slice_in_dim(padded_gain, order.astype(jnp.int32), L, 0)
        kept = jnp.arange(L, dtype=jnp.int32) < (L - order).astype(jnp.int32)
        filtered = jnp.where(kept[:, None, None], spec.reshape(L, 2, C) * gain_rows[:, None, :], jnp.float32(0.0)).astype(jnp.bfloat16)
        mixed = jnp.dot(filtered.reshape(2 * L, C).astype(jnp.float32), mix_wide, precision=high, preferred_element_type=jnp.float32)
        mixed = mixed.astype(jnp.bfloat16).reshape(L, 2 * C)
        synth = jnp.dot(table_wide.T, mixed.astype(jnp.float32), precision=high, preferred_element_type=jnp.float32)
        return synth.astype(jnp.bfloat16)
    synth = lax.map(per_slot, (legendre, fourier, slot_order))
    synth = synth.reshape(M, NLAT, 2, C).transpose(3, 1, 2, 0).reshape(C * NLAT, 2 * M)
    back = jnp.dot(synth.astype(jnp.float32), inverse.astype(jnp.float32), precision=high, preferred_element_type=jnp.float32)
    back = back.reshape(C, NLAT, NLON)
    return (state_field.astype(jnp.float32) + jax.nn.gelu(back, approximate=True)).astype(jnp.bfloat16)
```

```python
import functools
import math

import jax
import jax.numpy as jnp
from jax import lax
from jax.experimental import pallas as pl
from jax.experimental.pallas import tpu as pltpu
from jax.sharding import PartitionSpec as P

MESH = pl.DeviceIdType.MESH
BF = jnp.bfloat16
F32 = jnp.float32
LON = 1440
LONP = 1536
NX = 4
NO = 16
ND = NX * NO
MY = 8
PAIRS = 8
LAT = 180
DEG = 720
WIDE = 768
VLIM = 64 * 2**20 - 65536


def nn(a, b):
    return lax.dot_general(a, b, (((1,), (0,)), ((), ())), preferred_element_type=F32)


def nt(a, b):
    return lax.dot_general(a, b, (((1,), (1,)), ((), ())), preferred_element_type=F32)


def one_hot(cond):
    return jnp.where(cond, 1.0, 0.0).astype(BF)


def iota(shape, dim):
    return lax.broadcasted_iota(jnp.int32, shape, dim)


def cos_phase(p):
    p = p - jnp.floor(p * (1.0 / LON)) * LON
    a = (jnp.abs(p - LON / 2) - LON / 4) * (2.0 * math.pi / LON)
    z = a * a
    s = -1.0 / 39916800.0
    for c in (1.0 / 362880.0, -1.0 / 5040.0, 1.0 / 120.0, -1.0 / 6.0):
        s = s * z + c
    return a + a * (z * s)


def shuffle_matrix(transposed):
    i = iota((256, 256), 1 if transposed else 0)
    j = iota((256, 256), 0 if transposed else 1)
    src = (i % 8) * 32 + (i // 16) * 2 + (i // 8) % 2
    return one_hot(src == j)


def prologue_kernel(m_ref, gain_ref, mix_ref, gains_ref, mix2_ref):
    for i in range(MY):
        m = m_ref[i]
        rows = gain_ref[pl.ds(pl.multiple_of(m // 8 * 8, 8), WIDE + 8), :]
        rows = pltpu.roll(rows, lax.rem(WIDE + 8 - lax.rem(m, 8), WIDE + 8), 0)[0:WIDE]
        t = rows.T * jnp.where(m == 0, 1.0, 2.0)
        for h in range(2):
            for o in range(NO):
                at = (h * NO + o) * 8
                gains_ref[i, at : at + 8, :] = t[o * 16 + h * 8 : o * 16 + h * 8 + 8, :]
    i = iota((512, 256), 0)
    c = (i // 16) % NO * 16 + (i // 256) * 8 + i % 8
    j = iota((512, 256), 1)
    acc = jnp.zeros((512, 512), F32)
    for r in range(2):
        e = one_hot((c == j) & ((i // 8) % 2 == r))
        half = nt(e, mix_ref[...]).astype(BF)
        acc = acc + nt(half, e)
    mix2_ref[...] = acc.astype(BF)


def prologue(orders_here, degree_gain, mixing):
    padded = jnp.pad(degree_gain, ((0, 1288 - DEG), (0, 0)))
    vm = pl.BlockSpec(memory_space=pltpu.VMEM)
    return pl.pallas_call(
        prologue_kernel,
        out_shape=(
            jax.ShapeDtypeStruct((MY, 256, WIDE), F32),
            jax.ShapeDtypeStruct((512, 512), BF),
        ),
        in_specs=[pl.BlockSpec(memory_space=pltpu.SMEM), vm, vm],
        out_specs=(vm, vm),
        compiler_params=pltpu.CompilerParams(vmem_limit_bytes=VLIM),
        name="prologue",
    )(orders_here, padded, mixing)


def make_table(m_ref, f_ref):
    n = m_ref.shape[0]
    m = m_ref[...].astype(F32)
    r = (iota((n, 1), 0) % 2).astype(F32) * (LON / 4)
    low = m * iota((n, 128), 1).astype(F32) + r
    high = m * (iota((n, 128), 1) * 128).astype(F32)
    root = 1.0 / math.sqrt(LON)
    c0, s0 = cos_phase(low) * root, cos_phase(low + 0.75 * LON) * root
    c1, s1 = cos_phase(high), cos_phase(high + 0.75 * LON)
    lane = iota((1, 128), 1)
    for t in range(LONP // 128):
        v = c0 * c1[:, t : t + 1] - s0 * s1[:, t : t + 1]
        if t == LONP // 128 - 1:
            v = jnp.where(lane < LON - t * 128, v, 0.0)
        f_ref[:, t * 128 : (t + 1) * 128] = v.astype(BF)


def fill_grid(x_ref, xb):
    xb[:, :, LON:] = jnp.zeros((PAIRS, 384, LONP - LON), BF)
    xb[:, 304:320, :] = jnp.zeros((PAIRS, 16, LONP), BF)
    xb[:, 368:384, :] = jnp.zeros((PAIRS, 16, LONP), BF)

    def body(p, _):
        for h in range(2):
            xb[p, h * 128 : h * 128 + 128, 0:LON] = x_ref[h * 8 + p, 0:128, :]
            at = 256 + 64 * h
            xb[p, at : at + 52, 0:LON] = x_ref[h * 8 + p, 128:180, :]
        return 0

    lax.fori_loop(0, PAIRS, body, 0)


def forward_chunk(g, f_ref, xb, yb, send_ref, shuffle):
    rows = f_ref[pl.ds(pl.multiple_of(g * 256, 256), 256), :]

    def body(p, _):
        y = nt(rows, xb[p]).astype(BF)
        for q in range(8):
            yb[q, pl.ds(pl.multiple_of(p * 32, 32), 32), :] = y[q * 32 : q * 32 + 32, :]
        return 0

    lax.fori_loop(0, PAIRS, body, 0)
    for q in range(8):
        send_ref[2 * g + q // 4, q % 4] = nn(shuffle, yb[q]).astype(BF)


def forward_kernel(m_ref, x_ref, send_ref, f_ref, xb, yb):
    make_table(m_ref, f_ref)
    fill_grid(x_ref, xb)
    shuffle = shuffle_matrix(False)

    def body(g, _):
        forward_chunk(g, f_ref, xb, yb, send_ref, shuffle)
        return 0

    lax.fori_loop(0, 4, body, 0)


def forward(order_rows, state):
    vm = pl.BlockSpec(memory_space=pltpu.VMEM)
    return pl.pallas_call(
        forward_kernel,
        out_shape=(
            jax.ShapeDtypeStruct((MY, NX, 256, 384), BF),
            jax.ShapeDtypeStruct((2 * MY * ND, LONP), BF),
        ),
        in_specs=[vm, vm],
        out_specs=(vm, vm),
        scratch_shapes=[
            pltpu.VMEM((PAIRS, 384, LONP), BF),
            pltpu.VMEM((8, 256, 384), BF),
        ],
        compiler_params=pltpu.CompilerParams(vmem_limit_bytes=VLIM),
        name="forward",
    )(order_rows, state)


def greet():
    barrier = pltpu.get_barrier_semaphore()
    me = lax.axis_index("lat") * NO + lax.axis_index("ord")

    def body(k, _):
        d = lax.rem(me + k, ND)
        pl.semaphore_signal(
            barrier,
            inc=1,
            device_id={"lat": d // NO, "ord": lax.rem(d, NO)},
            device_id_type=MESH,
        )
        return 0

    lax.fori_loop(1, ND, body, 0)
    pl.semaphore_wait(barrier, ND - 1)


def partner(k, x, o):
    y, z = o // 4, lax.rem(o, 4)
    dx = lax.rem(x + k // 16, 4)
    dy = lax.rem(y + lax.rem(k // 4, 4), 4)
    dz = lax.rem(z + lax.rem(k, 4), 4)
    return dx, dy * 4 + dz


def send_slot(s, src, dst, send_sem, recv_sem, own_sem):
    x, o = lax.axis_index("lat"), lax.axis_index("ord")
    me = x * NO + o

    def body(k, _):
        dx, do = partner(k, x, o)
        pltpu.make_async_remote_copy(
            src_ref=src.at[s, dx * NO + do],
            dst_ref=dst.at[s, me],
            send_sem=send_sem,
            recv_sem=recv_sem.at[s],
            device_id={"lat": dx, "ord": do},
            device_id_type=MESH,
        ).start()
        return 0

    lax.fori_loop(1, ND, body, 0)
    pltpu.make_async_copy(src.at[s, me], dst.at[s, me], own_sem.at[s]).start()


def wait_slot(s, dst, recv_sem, own_sem):
    me = lax.axis_index("lat") * NO + lax.axis_index("ord")
    pltpu.make_async_copy(dst.at[s, me], dst.at[s, me], own_sem.at[s]).wait()
    others = dst.at[s, 0 : ND - 1]
    pltpu.make_async_copy(others, others, recv_sem.at[s]).wait()


def wait_sent(src, send_sem):
    others = src.at[:, 0 : ND - 1]
    pltpu.make_async_copy(others, others, send_sem).wait()


def exchange_kernel(src, dst, send_sem, recv_sem, own_sem):
    greet()
    for s in range(MY):
        send_slot(s, src, dst, send_sem, recv_sem, own_sem)
    for s in range(MY):
        wait_slot(s, dst, recv_sem, own_sem)
    wait_sent(src, send_sem)


def exchange(a, which):
    hbm = pl.BlockSpec(memory_space=pl.ANY)
    return pl.pallas_call(
        exchange_kernel,
        out_shape=jax.ShapeDtypeStruct(a.shape, a.dtype),
        in_specs=[hbm],
        out_specs=hbm,
        scratch_shapes=[
            pltpu.SemaphoreType.DMA,
            pltpu.SemaphoreType.DMA((MY,)),
            pltpu.SemaphoreType.DMA((MY,)),
        ],
        compiler_params=pltpu.CompilerParams(collective_id=which, has_side_effects=True),
        name=f"exchange_{which}",
    )(a)


def lat_select():
    row = iota((DEG, WIDE), 0)
    n = iota((DEG, WIDE), 1)
    tail = n - 512
    main = (n // 128) * LAT + n % 128
    rest = jnp.where(tail % 64 < 52, (tail // 64) * LAT + 128 + tail % 64, -1)
    return one_hot(row == jnp.where(n < 512, main, rest))


def slot_math(got, leg, gain, mix2, out):
    lane = iota((1, 128), 1)
    parts = [got(x) for x in range(NX)]
    rest = [v[:, 256:384].astype(F32) for v in parts]
    turned = [pltpu.roll(v, 64, 1) for v in rest]
    halves = []
    for h in range(2):
        cols = [v[:, h * 128 : h * 128 + 128] for v in parts]
        for x in (0, 2):
            a = rest[x] if h == 0 else turned[x]
            b = turned[x + 1] if h == 0 else rest[x + 1]
            cols.append(jnp.where(lane < 64, a, b).astype(BF))
        spec = nt(jnp.concatenate(cols, axis=1), leg)
        spec = spec.reshape(NO, 2, 8, WIDE) * gain[h * 128 : h * 128 + 128].reshape(NO, 1, 8, WIDE)
        halves.append(spec.reshape(256, WIDE).astype(BF))
    filtered = jnp.concatenate(halves, axis=0)
    syn = []
    for h in range(2):
        mixed = nn(mix2[h * 256 : h * 256 + 256], filtered).astype(BF)
        syn.append(nn(mixed, leg))
    for x in range(NX):
        at = 512 + (x // 2) * 128
        a, b = syn[0][:, at : at + 128], syn[1][:, at : at + 128]
        if x % 2:
            a = pltpu.roll(a, 64, 1)
        else:
            b = pltpu.roll(b, 64, 1)
        cols = [v[:, x * 128 : x * 128 + 128] for v in syn] + [jnp.where(lane < 64, a, b)]
        out(x, jnp.concatenate(cols, axis=1).astype(BF))


def middle_kernel(g_ref, leg_ref, gain_ref, mix2_ref, s_ref, legp, select):
    @pl.when(pl.program_id(0) == 0)
    def _():
        legp[DEG:WIDE, :] = jnp.zeros((WIDE - DEG, WIDE), BF)
        select[...] = lat_select()

    legp[0:DEG, :] = nn(leg_ref[0], select[...]).astype(BF)

    def out(x, v):
        s_ref[0, x] = v

    slot_math(lambda x: g_ref[0, x], legp[...], gain_ref[0], mix2_ref[...], out)


def middle(g, legendre, gains, mix2):
    block = pl.BlockSpec((1, NX, 256, 384), lambda i: (i, 0, 0, 0))
    return pl.pallas_call(
        middle_kernel,
        grid=(MY,),
        out_shape=jax.ShapeDtypeStruct(g.shape, BF),
        in_specs=[
            block,
            pl.BlockSpec((1, DEG, DEG), lambda i: (i, 0, 0)),
            pl.BlockSpec((1, 256, WIDE), lambda i: (i, 0, 0)),
            pl.BlockSpec((512, 512), lambda i: (0, 0)),
        ],
        out_specs=block,
        scratch_shapes=[pltpu.VMEM((WIDE, WIDE), BF), pltpu.VMEM((DEG, WIDE), BF)],
        compiler_params=pltpu.CompilerParams(vmem_limit_bytes=VLIM),
        name="middle",
    )(g, legendre, gains, mix2)


def inverse_kernel(r_ref, f_ref, x_ref, out_ref, b):
    @pl.when(pl.program_id(0) == 0)
    def _():
        shuffle = shuffle_matrix(True)

        def body(i, _):
            v = nn(shuffle, r_ref[i // NX, lax.rem(i, NX)]).astype(BF)
            for p in range(PAIRS):
                b[p, pl.ds(pl.multiple_of(i * 32, 32), 32), :] = v[p * 32 : p * 32 + 32, :]
            return 0

        lax.fori_loop(0, MY * NX, body, 0)

    bt = b[pl.program_id(0)].T
    for n in range(3):
        lanes = slice(n * 512, min(n * 512 + 512, LON))
        back = nn(bt, f_ref[:, n * 512 : n * 512 + 512])[:, : lanes.stop - lanes.start]
        back = jax.nn.gelu(back, approximate=True)
        for h in range(2):
            for rows, at in ((slice(0, 128), h * 128), (slice(128, 180), 256 + 64 * h)):
                size = rows.stop - rows.start
                x = x_ref[h, 0, rows, lanes].astype(F32)
                out_ref[h, 0, rows, lanes] = (x + back[at : at + size]).astype(BF)


def inverse(r, f, state):
    grid_block = pl.BlockSpec((2, 1, LAT, LON), lambda p: (0, p, 0, 0))
    whole = lambda shape: pl.BlockSpec(shape, lambda p: (0,) * len(shape))
    out = pl.pallas_call(
        inverse_kernel,
        grid=(PAIRS,),
        out_shape=jax.ShapeDtypeStruct((2, PAIRS, LAT, LON), BF),
        in_specs=[whole(r.shape), whole(f.shape), grid_block],
        out_specs=grid_block,
        scratch_shapes=[pltpu.VMEM((PAIRS, 2 * MY * ND, 384), BF)],
        compiler_params=pltpu.CompilerParams(vmem_limit_bytes=VLIM),
        name="inverse",
    )(r, f, state.reshape(2, PAIRS, LAT, LON))
    return out.reshape(2 * PAIRS, LAT, LON)


def shards(state_field, slot_order, legendre, degree_gain, mixing):
    me = lax.axis_index(("lat", "ord"))
    orders_here = lax.dynamic_slice_in_dim(slot_order, me * MY, MY, 0)
    order_rows = jnp.repeat(slot_order.reshape(ND, MY).T.reshape(-1), 2)[:, None]
    gains, mix2 = prologue(orders_here, degree_gain, mixing)
    send, table = forward(order_rows, state_field)
    got = exchange(send.reshape(MY, ND, 16, 384), 0).reshape(send.shape)
    answer = middle(got, legendre, gains, mix2)
    returned = exchange(answer.reshape(MY, ND, 16, 384), 1).reshape(send.shape)
    return inverse(returned, table, state_field)


def solution(mesh):
    placed = (P(("batch", "ord"), "lat", None), P(), P(("lat", "ord"), None, None), P(), P())
    return jax.shard_map(
        shards,
        mesh=mesh,
        in_specs=placed,
        out_specs=P(("batch", "ord"), "lat", None),
        check_vma=False,
    )
```

```python
import functools
import math

import jax
import jax.numpy as jnp
from jax import lax
from jax.experimental import pallas as pl
from jax.experimental.pallas import tpu as pltpu
from jax.sharding import PartitionSpec as P

MESH = pl.DeviceIdType.MESH
BF = jnp.bfloat16
F32 = jnp.float32
LON = 1440
LONP = 1536
NX = 4
NO = 16
ND = NX * NO
MY = 8
PAIRS = 8
LAT = 180
DEG = 720
WIDE = 768
VLIM = 64 * 2**20 - 65536


def nn(a, b):
    return lax.dot_general(a, b, (((1,), (0,)), ((), ())), preferred_element_type=F32)


def nt(a, b):
    return lax.dot_general(a, b, (((1,), (1,)), ((), ())), preferred_element_type=F32)


def one_hot(cond):
    return jnp.where(cond, 1.0, 0.0).astype(BF)


def iota(shape, dim):
    return lax.broadcasted_iota(jnp.int32, shape, dim)


def cos_phase(p):
    p = p - jnp.floor(p * (1.0 / LON)) * LON
    a = (jnp.abs(p - LON / 2) - LON / 4) * (2.0 * math.pi / LON)
    z = a * a
    s = -1.0 / 39916800.0
    for c in (1.0 / 362880.0, -1.0 / 5040.0, 1.0 / 120.0, -1.0 / 6.0):
        s = s * z + c
    return a + a * (z * s)


def shuffle_matrix(transposed):
    i = iota((256, 256), 1 if transposed else 0)
    j = iota((256, 256), 0 if transposed else 1)
    src = (i % 8) * 32 + (i // 16) * 2 + (i // 8) % 2
    return one_hot(src == j)


def greet_signal():
    barrier = pltpu.get_barrier_semaphore()
    me = lax.axis_index("lat") * NO + lax.axis_index("ord")

    def body(k, _):
        d = lax.rem(me + k, ND)
        pl.semaphore_signal(
            barrier,
            inc=1,
            device_id={"lat": d // NO, "ord": lax.rem(d, NO)},
            device_id_type=MESH,
        )
        return 0

    lax.fori_loop(1, ND, body, 0)


def greet_wait():
    pl.semaphore_wait(pltpu.get_barrier_semaphore(), ND - 1)


def partner(k, x, o):
    y, z = o // 4, lax.rem(o, 4)
    dx = lax.rem(x + k // 16, 4)
    dy = lax.rem(y + lax.rem(k // 4, 4), 4)
    dz = lax.rem(z + lax.rem(k, 4), 4)
    return dx, dy * 4 + dz


def send_slot(s, src, dst, send_sem, recv_sem, own_sem):
    x, o = lax.axis_index("lat"), lax.axis_index("ord")
    me = x * NO + o

    def body(k, _):
        dx, do = partner(k, x, o)
        pltpu.make_async_remote_copy(
            src_ref=src.at[s, dx * NO + do],
            dst_ref=dst.at[s, me],
            send_sem=send_sem,
            recv_sem=recv_sem.at[s],
            device_id={"lat": dx, "ord": do},
            device_id_type=MESH,
        ).start()
        return 0

    lax.fori_loop(1, ND, body, 0)
    pltpu.make_async_copy(src.at[s, me], dst.at[s, me], own_sem.at[s]).start()


def wait_slot(s, dst, recv_sem, own_sem):
    me = lax.axis_index("lat") * NO + lax.axis_index("ord")
    pltpu.make_async_copy(dst.at[s, me], dst.at[s, me], own_sem.at[s]).wait()
    others = dst.at[s, 0 : ND - 1]
    pltpu.make_async_copy(others, others, recv_sem.at[s]).wait()


def wait_sent(src, send_sem):
    others = src.at[:, 0 : ND - 1]
    pltpu.make_async_copy(others, others, send_sem).wait()


def lat_select():
    row = iota((DEG, WIDE), 0)
    n = iota((DEG, WIDE), 1)
    tail = n - 512
    main = (n // 128) * LAT + n % 128
    rest = jnp.where(tail % 64 < 52, (tail // 64) * LAT + 128 + tail % 64, -1)
    return one_hot(row == jnp.where(n < 512, main, rest))


def slot_math(got, leg, gain, mix2, out):
    lane = iota((1, 128), 1)
    parts = [got(x) for x in range(NX)]
    rest = [v[:, 256:384].astype(F32) for v in parts]
    turned = [pltpu.roll(v, 64, 1) for v in rest]
    halves = []
    for h in range(2):
        cols = [v[:, h * 128 : h * 128 + 128] for v in parts]
        for x in (0, 2):
            a = rest[x] if h == 0 else turned[x]
            b = turned[x + 1] if h == 0 else rest[x + 1]
            cols.append(jnp.where(lane < 64, a, b).astype(BF))
        spec = nt(jnp.concatenate(cols, axis=1), leg)
        spec = spec.reshape(NO, 2, 8, WIDE) * gain[h * 128 : h * 128 + 128].reshape(NO, 1, 8, WIDE)
        halves.append(spec.reshape(256, WIDE).astype(BF))
    filtered = jnp.concatenate(halves, axis=0)
    syn = []
    for h in range(2):
        mixed = nn(mix2[h * 256 : h * 256 + 256, :], filtered).astype(BF)
        syn.append(nn(mixed, leg))
    for x in range(NX):
        at = 512 + (x // 2) * 128
        a, b = syn[0][:, at : at + 128], syn[1][:, at : at + 128]
        if x % 2:
            a = pltpu.roll(a, 64, 1)
        else:
            b = pltpu.roll(b, 64, 1)
        cols = [v[:, x * 128 : x * 128 + 128] for v in syn] + [jnp.where(lane < 64, a, b)]
        out(x, jnp.concatenate(cols, axis=1).astype(BF))


def swap_matrix():
    i = iota((256, 256), 0)
    j = iota((256, 256), 1)
    return one_hot((i % 16) * 16 + i // 16 == j)


def lat_rows(g, h):
    return h * 128 + g * 16 if g < 8 else 256 + h * 64 + (g - 8) * 16


def table_columns(order_ref):
    rep = one_hot(iota((128, ND), 0) // 2 == iota((128, ND), 1))
    m = order_ref[...]
    low = nn(rep, (m % 256).astype(F32).astype(BF))
    high = nn(rep, (m // 256).astype(F32).astype(BF))
    return low + 256.0 * high


def make_table(s, columns, f_ref):
    m = columns[:, s : s + 1]
    r = (iota((128, 1), 0) % 2).astype(F32) * (LON / 4)
    low = m * iota((128, 128), 1).astype(F32) + r
    high = m * (iota((128, 128), 1) * 128).astype(F32)
    root = 1.0 / math.sqrt(LON)
    c0, s0 = cos_phase(low) * root, cos_phase(low + 0.75 * LON) * root
    c1, s1 = cos_phase(high), cos_phase(high + 0.75 * LON)
    lane = iota((1, 128), 1)
    for t in range(LONP // 128):
        v = c0 * c1[:, t : t + 1] - s0 * s1[:, t : t + 1]
        if t == LONP // 128 - 1:
            v = jnp.where(lane < LON - t * 128, v, 0.0)
        f_ref[s * 128 : s * 128 + 128, t * 128 : (t + 1) * 128] = v.astype(BF)


def fill_grid(xs, xb, swap):
    def body(g, _):
        v = nn(swap, xs[pl.ds(g * 16, 16)].reshape(256, LON)).astype(BF)
        for c in range(16):
            h = c // 8
            at = jnp.where(g < 8, h * 128 + g * 16, 256 + h * 64 + (g - 8) * 16)
            xb[c % 8, pl.ds(pl.multiple_of(at, 16), 16), 0:LON] = v[c * 16 : c * 16 + 16]
        return 0

    lax.fori_loop(0, 12, body, 0)


def forward_chunk(g, f_ref, xb, yb, send, shuffle):
    rows = f_ref[pl.ds(pl.multiple_of(g * 256, 256), 256), :]

    def body(p, _):
        y = nt(rows, xb[p]).astype(BF)
        for q in range(8):
            yb[q, pl.ds(pl.multiple_of(p * 32, 32), 32), :] = y[q * 32 : q * 32 + 32, :]
        return 0

    lax.fori_loop(0, PAIRS, body, 0)
    for q in range(8):
        v = nn(shuffle, yb[q]).astype(BF)
        send[2 * g + q // 4, (q % 4) * 16 : (q % 4) * 16 + 16] = v.reshape(16, 16, 384)


def split_gain(gain_ref, gp):
    gp[:, DEG:] = jnp.zeros((768, WIDE - DEG), BF)
    t = gain_ref[...].T
    for piece in range(3):
        part = t.astype(BF)
        t = t - part.astype(F32)
        for h in range(2):
            for o in range(NO):
                at = piece * 256 + (h * NO + o) * 8
                gp[at : at + 8, 0:DEG] = part[o * 16 + h * 8 : o * 16 + h * 8 + 8, :]


def slot_gain(m, gp, gs):
    pick = one_hot(iota((WIDE, WIDE), 0) == iota((WIDE, WIDE), 1) + m)
    v = nn(gp[...], pick)
    weight = jnp.where(jnp.full((1, WIDE), m, jnp.int32) == 0, 1.0, 2.0)
    gs[...] = (v[0:256] + v[256:512] + v[512:768]) * weight


def two_part_mixing(mix_ref, mix2):
    i = iota((512, 256), 0)
    c = (i // 16) % NO * 16 + (i // 256) * 8 + i % 8
    j = iota((512, 256), 1)
    acc = jnp.zeros((512, 512), F32)
    for r in range(2):
        e = one_hot(c + 256 * ((i // 8) % 2) == j + 256 * r)
        half = nt(e, mix_ref[...]).astype(BF)
        acc = acc + nt(half, e)
    mix2[...] = acc.astype(BF)


def collect(s, ret, bb, tb, lb, shuffle_back, swap):
    for x in range(NX):
        v = nn(shuffle_back, ret[s, x * 16 : x * 16 + 16].reshape(256, 384)).astype(BF)
        for p in range(PAIRS):
            bb[p, x * 32 : x * 32 + 32, :] = v[p * 32 : p * 32 + 32, :]

    def turn(p, _):
        t = bb[p].T
        for h in range(2):
            for g in range(12):
                at = lat_rows(g, h)
                tb[g, pl.ds(pl.multiple_of(h * 128 + p * 16, 16), 16), :] = t[at : at + 16]
        return 0

    lax.fori_loop(0, PAIRS, turn, 0)

    def place(g, _):
        lb[pl.ds(pl.multiple_of(g * 256, 256), 256), :] = nn(swap, tb[g]).astype(BF)
        return 0

    lax.fori_loop(0, 12, place, 0)


def transform_kernel(
    so_ref, order_ref, gain_ref, mix_ref, x_hbm, leg_hbm,
    l_hbm, f_hbm,
    xs, xb, fb, yb, send, got, ans, ret, leg, legp, select, gp, gs, mix2, bb, tb, lb,
    x_sem, leg_sem, f_sem, l_sem, send_sem, recv_sem, own_sem, send2_sem, recv2_sem, own2_sem,
):
    me = lax.axis_index("lat") * NO + lax.axis_index("ord")
    load_x = pltpu.make_async_copy(x_hbm, xs.at[0:LAT], x_sem)
    load_x.start()

    def load_leg(s):
        return pltpu.make_async_copy(leg_hbm.at[s], leg.at[lax.rem(s, 2)], leg_sem.at[lax.rem(s, 2)])

    load_leg(0).start()
    load_leg(1).start()
    greet_signal()
    columns = table_columns(order_ref)
    for s in range(2):
        make_table(s, columns, fb)
    shuffle = shuffle_matrix(False)
    swap = swap_matrix()
    xs[LAT:192] = jnp.zeros((192 - LAT, 16, LON), BF)
    xb[:, :, LON:] = jnp.zeros((PAIRS, 384, LONP - LON), BF)
    load_x.wait()
    fill_grid(xs, xb, swap)
    forward_chunk(0, fb, xb, yb, send, shuffle)
    greet_wait()
    for s in range(2):
        send_slot(s, send, got, send_sem, recv_sem, own_sem)
    for s in range(2, MY):
        make_table(s, columns, fb)
    save_f = pltpu.make_async_copy(fb, f_hbm, f_sem)
    save_f.start()

    def chunk(g, _):
        forward_chunk(g, fb, xb, yb, send, shuffle)
        send_slot(2 * g, send, got, send_sem, recv_sem, own_sem)
        send_slot(2 * g + 1, send, got, send_sem, recv_sem, own_sem)
        return 0

    lax.fori_loop(1, 4, chunk, 0)

    two_part_mixing(mix_ref, mix2)
    split_gain(gain_ref, gp)
    select[...] = lat_select()
    legp[DEG:WIDE, :] = jnp.zeros((WIDE - DEG, WIDE), BF)

    def slot(s, _):
        slot_gain(so_ref[me * MY + s], gp, gs)
        load_leg(s).wait()
        legp[0:DEG, :] = nn(leg[lax.rem(s, 2)], select[...]).astype(BF)

        @pl.when(s + 2 < MY)
        def _():
            load_leg(s + 2).start()

        wait_slot(s, got, recv_sem, own_sem)

        def out(x, v):
            ans[s, x * 16 : x * 16 + 16] = v.reshape(16, 16, 384)

        slot_math(
            lambda x: got[s, x * 16 : x * 16 + 16].reshape(256, 384), legp[...], gs[...], mix2, out
        )
        send_slot(s, ans, ret, send2_sem, recv2_sem, own2_sem)
        return 0

    lax.fori_loop(0, MY, slot, 0)

    shuffle_back = shuffle_matrix(True)

    def save_l(s):
        at = pl.ds(pl.multiple_of(s * 128, 128), 128)
        return pltpu.make_async_copy(
            lb.at[lax.rem(s, 2), 0 : LAT * 16], l_hbm.at[:, at], l_sem.at[lax.rem(s, 2)]
        )

    def back(s, _):
        wait_slot(s, ret, recv2_sem, own2_sem)

        @pl.when(s >= 2)
        def _():
            save_l(s - 2).wait()

        collect(s, ret, bb, tb, lb.at[lax.rem(s, 2)], shuffle_back, swap)
        save_l(s).start()
        return 0

    lax.fori_loop(0, MY, back, 0)
    save_l(MY - 2).wait()
    save_l(MY - 1).wait()
    save_f.wait()
    wait_sent(send, send_sem)
    wait_sent(ans, send2_sem)


def transform(slot_order, degree_gain, mixing, state, legendre):
    vm = pl.BlockSpec(memory_space=pltpu.VMEM)
    hbm = pl.BlockSpec(memory_space=pl.ANY)
    dma = pltpu.SemaphoreType.DMA
    message = pltpu.VMEM((MY, ND, 16, 384), BF)
    return pl.pallas_call(
        transform_kernel,
        out_shape=(
            jax.ShapeDtypeStruct((LAT * 16, 2 * MY * ND), BF),
            jax.ShapeDtypeStruct((2 * MY * ND, LONP), BF),
        ),
        in_specs=[pl.BlockSpec(memory_space=pltpu.SMEM), vm, vm, vm, hbm, hbm],
        out_specs=(hbm, hbm),
        scratch_shapes=[
            pltpu.VMEM((192, 16, LON), BF),
            pltpu.VMEM((PAIRS, 384, LONP), BF),
            pltpu.VMEM((2 * MY * ND, LONP), BF),
            pltpu.VMEM((8, 256, 384), BF),
            message,
            message,
            message,
            message,
            pltpu.VMEM((2, DEG, DEG), BF),
            pltpu.VMEM((WIDE, WIDE), BF),
            pltpu.VMEM((DEG, WIDE), BF),
            pltpu.VMEM((768, WIDE), BF),
            pltpu.VMEM((256, WIDE), F32),
            pltpu.VMEM((512, 512), BF),
            pltpu.VMEM((PAIRS, 128, 384), BF),
            pltpu.VMEM((12, 256, 128), BF),
            pltpu.VMEM((2, 3072, 128), BF),
            dma,
            dma((2,)),
            dma,
            dma((2,)),
            dma,
            dma((MY,)),
            dma((MY,)),
            dma,
            dma((MY,)),
            dma((MY,)),
        ],
        compiler_params=pltpu.CompilerParams(
            collective_id=0, has_side_effects=True, vmem_limit_bytes=VLIM
        ),
        name="transform",
    )(slot_order, slot_order.reshape(ND, MY), degree_gain, mixing, state, legendre)


ROWS = 288


def inverse_kernel(l_ref, f_ref, x_ref, out_ref):
    for n in range(3):
        lanes = slice(n * 512, min(n * 512 + 512, LON))
        back = nn(l_ref[...], f_ref[:, n * 512 : n * 512 + 512])[:, : lanes.stop - lanes.start]
        back = jax.nn.gelu(back, approximate=True)
        out_ref[:, lanes] = (x_ref[:, lanes].astype(F32) + back).astype(BF)


def inverse(l, f, state):
    rows = lambda width: pl.BlockSpec((ROWS, width), lambda i: (i, 0))
    return pl.pallas_call(
        inverse_kernel,
        grid=(LAT * 16 // ROWS,),
        out_shape=jax.ShapeDtypeStruct((LAT * 16, LON), BF),
        in_specs=[rows(2 * MY * ND), pl.BlockSpec(f.shape, lambda i: (0, 0)), rows(LON)],
        out_specs=rows(LON),
        compiler_params=pltpu.CompilerParams(vmem_limit_bytes=VLIM),
        name="inverse",
    )(l, f, state)


def shards(state_field, slot_order, legendre, degree_gain, mixing):
    state = state_field.transpose(1, 0, 2)
    l, f = transform(slot_order, degree_gain, mixing, state, legendre)
    out = inverse(l, f, state.reshape(LAT * 16, LON))
    return out.reshape(LAT, 16, LON).transpose(1, 0, 2)


def solution(mesh):
    placed = (P(("batch", "ord"), "lat", None), P(), P(("lat", "ord"), None, None), P(), P())
    return jax.shard_map(
        shards,
        mesh=mesh,
        in_specs=placed,
        out_specs=P(("batch", "ord"), "lat", None),
        check_vma=False,
    )
```

```python
import functools
import math

import jax
import jax.numpy as jnp
from jax import lax
from jax.experimental import pallas as pl
from jax.experimental.pallas import tpu as pltpu
from jax.sharding import PartitionSpec as P

MESH = pl.DeviceIdType.MESH
BF = jnp.bfloat16
F32 = jnp.float32
LON = 1440
LONP = 1536
NX = 4
NO = 16
ND = NX * NO
MY = 8
PAIRS = 8
LAT = 180
DEG = 720
WIDE = 768
VLIM = 64 * 2**20 - 65536


def nn(a, b):
    return lax.dot_general(a, b, (((1,), (0,)), ((), ())), preferred_element_type=F32)


def nt(a, b):
    return lax.dot_general(a, b, (((1,), (1,)), ((), ())), preferred_element_type=F32)


def one_hot(cond):
    return jnp.where(cond, 1.0, 0.0).astype(BF)


def iota(shape, dim):
    return lax.broadcasted_iota(jnp.int32, shape, dim)


def cos_phase(p):
    p = p - jnp.floor(p * (1.0 / LON)) * LON
    a = (jnp.abs(p - LON / 2) - LON / 4) * (2.0 * math.pi / LON)
    z = a * a
    s = -1.0 / 39916800.0
    for c in (1.0 / 362880.0, -1.0 / 5040.0, 1.0 / 120.0, -1.0 / 6.0):
        s = s * z + c
    return a + a * (z * s)


def shuffle_matrix(transposed):
    i = iota((256, 256), 1 if transposed else 0)
    j = iota((256, 256), 0 if transposed else 1)
    src = (i % 8) * 32 + (i // 16) * 2 + (i // 8) % 2
    return one_hot(src == j)


def greet_signal():
    barrier = pltpu.get_barrier_semaphore()
    me = lax.axis_index("lat") * NO + lax.axis_index("ord")

    def body(k, _):
        d = lax.rem(me + k, ND)
        pl.semaphore_signal(
            barrier,
            inc=1,
            device_id={"lat": d // NO, "ord": lax.rem(d, NO)},
            device_id_type=MESH,
        )
        return 0

    lax.fori_loop(1, ND, body, 0)


def greet_wait():
    pl.semaphore_wait(pltpu.get_barrier_semaphore(), ND - 1)


def partner(k, x, o):
    y, z = o // 4, lax.rem(o, 4)
    dx = lax.rem(x + k // 16, 4)
    dy = lax.rem(y + lax.rem(k // 4, 4), 4)
    dz = lax.rem(z + lax.rem(k, 4), 4)
    return dx, dy * 4 + dz


def send_slot(s, src, dst, send_sem, recv_sem, own_sem):
    x, o = lax.axis_index("lat"), lax.axis_index("ord")
    me = x * NO + o

    def body(k, _):
        dx, do = partner(k, x, o)
        pltpu.make_async_remote_copy(
            src_ref=src.at[s, dx * NO + do],
            dst_ref=dst.at[s, me],
            send_sem=send_sem,
            recv_sem=recv_sem.at[s],
            device_id={"lat": dx, "ord": do},
            device_id_type=MESH,
        ).start()
        return 0

    lax.fori_loop(1, ND, body, 0)
    pltpu.make_async_copy(src.at[s, me], dst.at[s, me], own_sem.at[s]).start()


def wait_slot(s, dst, recv_sem, own_sem):
    me = lax.axis_index("lat") * NO + lax.axis_index("ord")
    pltpu.make_async_copy(dst.at[s, me], dst.at[s, me], own_sem.at[s]).wait()
    others = dst.at[s, 0 : ND - 1]
    pltpu.make_async_copy(others, others, recv_sem.at[s]).wait()


def wait_sent(src, send_sem):
    others = src.at[:, 0 : ND - 1]
    pltpu.make_async_copy(others, others, send_sem).wait()


def lat_select():
    row = iota((DEG, WIDE), 0)
    n = iota((DEG, WIDE), 1)
    tail = n - 512
    main = (n // 128) * LAT + n % 128
    rest = jnp.where(tail % 64 < 52, (tail // 64) * LAT + 128 + tail % 64, -1)
    return one_hot(row == jnp.where(n < 512, main, rest))


def slot_math(got, leg, gain, mix2, out):
    lane = iota((1, 128), 1)
    parts = [got(x) for x in range(NX)]
    rest = [v[:, 256:384].astype(F32) for v in parts]
    turned = [pltpu.roll(v, 64, 1) for v in rest]
    halves = []
    for h in range(2):
        cols = [v[:, h * 128 : h * 128 + 128] for v in parts]
        for x in (0, 2):
            a = rest[x] if h == 0 else turned[x]
            b = turned[x + 1] if h == 0 else rest[x + 1]
            cols.append(jnp.where(lane < 64, a, b).astype(BF))
        spec = nt(jnp.concatenate(cols, axis=1), leg)
        spec = spec.reshape(NO, 2, 8, WIDE) * gain[h * 128 : h * 128 + 128].reshape(NO, 1, 8, WIDE)
        halves.append(spec.reshape(256, WIDE).astype(BF))
    filtered = jnp.concatenate(halves, axis=0)
    syn = []
    for h in range(2):
        mixed = nn(mix2[h * 256 : h * 256 + 256, :], filtered).astype(BF)
        syn.append(nn(mixed, leg))
    for x in range(NX):
        at = 512 + (x // 2) * 128
        a, b = syn[0][:, at : at + 128], syn[1][:, at : at + 128]
        if x % 2:
            a = pltpu.roll(a, 64, 1)
        else:
            b = pltpu.roll(b, 64, 1)
        cols = [v[:, x * 128 : x * 128 + 128] for v in syn] + [jnp.where(lane < 64, a, b)]
        out(x, jnp.concatenate(cols, axis=1).astype(BF))


def swap_matrix():
    i = iota((256, 256), 0)
    j = iota((256, 256), 1)
    return one_hot((i % 16) * 16 + i // 16 == j)


def lat_rows(g, h):
    return h * 128 + g * 16 if g < 8 else 256 + h * 64 + (g - 8) * 16


def table_orders(order_ref):
    d = iota((128, 128), 0) // 2
    m = jnp.zeros((128, 128), jnp.int32)
    for i in range(4):
        m = jnp.where(d // 16 == i, order_ref[i : i + 1, :], m)
    m = jnp.where(iota((128, 128), 1) // 8 == d % 16, m, 0)
    return (m % 256).astype(F32).astype(BF), (m // 256).astype(F32).astype(BF)


def make_table(s, orders, f_ref):
    take = one_hot(iota((128, 128), 0) % 8 == s)
    m = nn(orders[0], take) + 256.0 * nn(orders[1], take)
    r = (iota((128, 1), 0) % 2).astype(F32) * (LON / 4)
    low = m * iota((128, 128), 1).astype(F32) + r
    high = m * (iota((128, 128), 1) * 128).astype(F32)
    root = 1.0 / math.sqrt(LON)
    c0, s0 = cos_phase(low) * root, cos_phase(low + 0.75 * LON) * root
    c1, s1 = cos_phase(high), cos_phase(high + 0.75 * LON)
    lane = iota((1, 128), 1)
    for t in range(LONP // 128):
        v = c0 * c1[:, t : t + 1] - s0 * s1[:, t : t + 1]
        if t == LONP // 128 - 1:
            v = jnp.where(lane < LON - t * 128, v, 0.0)
        f_ref[pl.ds(pl.multiple_of(s * 128, 128), 128), t * 128 : (t + 1) * 128] = v.astype(BF)


def load_grid(g, x_hbm, xs, x_sem):
    part = pl.ds(g * 16, min(16, LAT - g * 16))
    return pltpu.make_async_copy(x_hbm.at[part], xs.at[part], x_sem.at[g])


def fill_grid(x_hbm, xs, xb, x_sem, swap):
    for g in range(12):
        load_grid(g, x_hbm, xs, x_sem).wait()
        v = nn(swap, xs[g * 16 : g * 16 + 16].reshape(256, LON)).astype(BF)
        for c in range(16):
            at = lat_rows(g, c // 8)
            xb[c % 8, at : at + 16, 0:LON] = v[c * 16 : c * 16 + 16]


def forward_slot(s, f_ref, xb, yb, send, shuffle):
    rows = f_ref[pl.ds(pl.multiple_of(s * 128, 128), 128), :]
    for p in range(PAIRS):
        y = nt(rows, xb[p]).astype(BF)
        for q in range(NX):
            yb[q, p * 32 : p * 32 + 32, :] = y[q * 32 : q * 32 + 32, :]
    for q in range(NX):
        v = nn(shuffle, yb[q]).astype(BF)
        send[s, q * 16 : q * 16 + 16] = v.reshape(16, 16, 384)


def split_gain(gain_ref, gp):
    gp[:, DEG:] = jnp.zeros((768, WIDE - DEG), BF)
    t = gain_ref[...].T
    for piece in range(3):
        part = t.astype(BF)
        t = t - part.astype(F32)
        for h in range(2):
            for o in range(NO):
                at = piece * 256 + (h * NO + o) * 8
                gp[at : at + 8, 0:DEG] = part[o * 16 + h * 8 : o * 16 + h * 8 + 8, :]


def slot_gain(m, gp, gs):
    pick = one_hot(iota((WIDE, WIDE), 0) == iota((WIDE, WIDE), 1) + m)
    v = nn(gp[...], pick)
    weight = jnp.where(jnp.full((1, WIDE), m, jnp.int32) == 0, 1.0, 2.0)
    gs[...] = (v[0:256] + v[256:512] + v[512:768]) * weight


def two_part_mixing(mix_ref, mix2):
    i = iota((512, 256), 0)
    c = (i // 16) % NO * 16 + (i // 256) * 8 + i % 8
    j = iota((512, 256), 1)
    acc = jnp.zeros((512, 512), F32)
    for r in range(2):
        e = one_hot(c + 256 * ((i // 8) % 2) == j + 256 * r)
        half = nt(e, mix_ref[...]).astype(BF)
        acc = acc + nt(half, e)
    mix2[...] = acc.astype(BF)


def collect(s, ret, bb, tb, lb, shuffle_back, swap):
    for x in range(NX):
        v = nn(shuffle_back, ret[s, x * 16 : x * 16 + 16].reshape(256, 384)).astype(BF)
        for p in range(PAIRS):
            bb[p, x * 32 : x * 32 + 32, :] = v[p * 32 : p * 32 + 32, :]

    for p in range(PAIRS):
        t = bb[p].T
        for h in range(2):
            for g in range(12):
                at = lat_rows(g, h)
                tb[g, h * 128 + p * 16 : h * 128 + p * 16 + 16, :] = t[at : at + 16]

    for g in range(12):
        lb[g * 256 : g * 256 + 256, :] = nn(swap, tb[g]).astype(BF)


LAST = MY - 2
BLOCK = 288
BLOCKS = LAT * 16 // BLOCK


def half_gelu(v):
    k = math.sqrt(2.0 / math.pi)
    h = 0.5 * v
    return h + h * jnp.tanh(v * (k + (k * 0.044715) * (v * v)))


def transform_kernel(
    so_ref, order_ref, gain_ref, mix_ref, x_hbm, leg_hbm,
    part_hbm, l_hbm, f_hbm,
    fb, send, got, ans, ret, leg, legp, select, gp, gs, mix2, bb, tb, lb,
    x_sem, leg_sem, out_sem, l_sem, f_sem,
    send_sem, recv_sem, own_sem, send2_sem, recv2_sem, own2_sem,
):
    me = lax.axis_index("lat") * NO + lax.axis_index("ord")
    swap = swap_matrix()

    def load_leg(s):
        return pltpu.make_async_copy(leg_hbm.at[s], leg.at[lax.rem(s, 2)], leg_sem.at[lax.rem(s, 2)])

    def first(xs, xb, yb):
        for g in range(12):
            load_grid(g, x_hbm, xs, x_sem).start()
        greet_signal()
        load_leg(0).start()
        load_leg(1).start()
        orders = table_orders(order_ref)
        shuffle = shuffle_matrix(False)
        xs[LAT:192] = jnp.zeros((192 - LAT, 16, LON), BF)
        xb[:, :, LON:] = jnp.zeros((PAIRS, 384, LONP - LON), BF)
        make_table(0, orders, fb)
        fill_grid(x_hbm, xs, xb, x_sem, swap)
        greet_wait()

        def slot(s, _):
            forward_slot(s, fb, xb, yb, send, shuffle)
            send_slot(s, send, got, send_sem, recv_sem, own_sem)

            @pl.when(s + 1 < MY)
            def _():
                make_table(s + 1, orders, fb)

            return 0

        lax.fori_loop(0, MY, slot, 0)

    pl.run_scoped(
        first,
        pltpu.VMEM((192, 16, LON), BF),
        pltpu.VMEM((PAIRS, 384, LONP), BF),
        pltpu.VMEM((NX, 256, 384), BF),
    )

    two_part_mixing(mix_ref, mix2)
    split_gain(gain_ref, gp)
    select[...] = lat_select()
    legp[DEG:WIDE, :] = jnp.zeros((WIDE - DEG, WIDE), BF)

    def slot(s, _):
        slot_gain(so_ref[me * MY + s], gp, gs)
        load_leg(s).wait()
        legp[0:DEG, :] = nn(leg[lax.rem(s, 2)], select[...]).astype(BF)

        @pl.when(s + 2 < MY)
        def _():
            load_leg(s + 2).start()

        wait_slot(s, got, recv_sem, own_sem)

        def out(x, v):
            ans[s, x * 16 : x * 16 + 16] = v.reshape(16, 16, 384)

        slot_math(
            lambda x: got[s, x * 16 : x * 16 + 16].reshape(256, 384), legp[...], gs[...], mix2, out
        )
        send_slot(s, ans, ret, send2_sem, recv2_sem, own2_sem)
        return 0

    lax.fori_loop(0, MY, slot, 0)

    save_f = pltpu.make_async_copy(fb.at[LAST * 128 :], f_hbm, f_sem)
    save_f.start()

    def last(acc, out):
        shuffle_back = shuffle_matrix(True)

        def block(i):
            return pl.ds(pl.multiple_of(i * BLOCK, 32), BLOCK)

        def save(i):
            at = lax.rem(i, 2)
            return pltpu.make_async_copy(out.at[at], part_hbm.at[block(i)], out_sem.at[at])

        def gather(s, k):
            wait_slot(s, ret, recv2_sem, own2_sem)
            collect(s, ret, bb, tb, lb.at[k], shuffle_back, swap)

        def product(t, i, n):
            v = jnp.concatenate([lb[0, block(i), :], lb[1, block(i), :]], axis=1)
            rows = pl.ds(pl.multiple_of(t * 256, 256), 256)
            return nn(v, fb[rows, n * 512 : n * 512 + 512])

        def add(t, start):
            def body(i, _):
                for n in range(3):
                    lanes = slice(n * 512, n * 512 + 512)
                    v = product(t, i, n)
                    acc[block(i), lanes] = v if start else acc[block(i), lanes] + v
                return 0

            lax.fori_loop(0, BLOCKS, body, 0)

        def finish(i, _):
            @pl.when(i >= 2)
            def _():
                save(i - 2).wait()

            for n in range(3):
                lo, hi = n * 512, min(n * 512 + 512, LON)
                v = acc[block(i), lo : lo + 512] + product(LAST // 2 - 1, i, n)
                out[lax.rem(i, 2), :, lo:hi] = v[:, : hi - lo].astype(BF)
            save(i).start()
            return 0

        for t in range(LAST // 2):
            gather(2 * t, 0)
            gather(2 * t + 1, 1)
            if t < LAST // 2 - 1:
                add(t, t == 0)
        lax.fori_loop(0, BLOCKS, finish, 0)
        for k in range(2):
            gather(LAST + k, k)
            save_l(k).start()
        save(BLOCKS - 2).wait()
        save(BLOCKS - 1).wait()

    def save_l(k):
        return pltpu.make_async_copy(lb.at[k, 0 : LAT * 16], l_hbm.at[k], l_sem.at[k])

    pl.run_scoped(
        last,
        pltpu.VMEM((LAT * 16, LONP), F32),
        pltpu.VMEM((2, BLOCK, LON), BF),
    )
    save_f.wait()
    save_l(0).wait()
    save_l(1).wait()
    wait_sent(send, send_sem)
    wait_sent(ans, send2_sem)


def transform(slot_order, degree_gain, mixing, state, legendre):
    vm = pl.BlockSpec(memory_space=pltpu.VMEM)
    hbm = pl.BlockSpec(memory_space=pl.ANY)
    dma = pltpu.SemaphoreType.DMA
    message = pltpu.VMEM((MY, ND, 16, 384), BF)
    return pl.pallas_call(
        transform_kernel,
        out_shape=(
            jax.ShapeDtypeStruct((LAT * 16, LON), BF),
            jax.ShapeDtypeStruct((2, LAT * 16, 128), BF),
            jax.ShapeDtypeStruct((256, LONP), BF),
        ),
        in_specs=[pl.BlockSpec(memory_space=pltpu.SMEM), vm, vm, vm, hbm, hbm],
        out_specs=(hbm, hbm, hbm),
        scratch_shapes=[
            pltpu.VMEM((2 * MY * ND, LONP), BF),
            message,
            message,
            message,
            message,
            pltpu.VMEM((2, DEG, DEG), BF),
            pltpu.VMEM((WIDE, WIDE), BF),
            pltpu.VMEM((DEG, WIDE), BF),
            pltpu.VMEM((768, WIDE), BF),
            pltpu.VMEM((256, WIDE), F32),
            pltpu.VMEM((512, 512), BF),
            pltpu.VMEM((PAIRS, 128, 384), BF),
            pltpu.VMEM((12, 256, 128), BF),
            pltpu.VMEM((2, 3072, 128), BF),
            dma((12,)),
            dma((2,)),
            dma((2,)),
            dma((2,)),
            dma,
            dma,
            dma((MY,)),
            dma((MY,)),
            dma,
            dma((MY,)),
            dma((MY,)),
        ],
        compiler_params=pltpu.CompilerParams(
            collective_id=0, has_side_effects=True, vmem_limit_bytes=VLIM
        ),
        name="transform",
    )(
        slot_order, slot_order.reshape(4, 128), degree_gain, mixing, state, legendre,
    )


ROWS = 480
STEPS = LAT * 16 // ROWS


def update_kernel(
    part_hbm, l_hbm, f_hbm, x_hbm, out_hbm,
    part, l, f, x, out, part_sem, l_sem, f_sem, x_sem, out_sem,
):
    def block(i):
        return pl.ds(pl.multiple_of(i * ROWS, 32), ROWS)

    def loads(i):
        at = block(i)
        return (
            pltpu.make_async_copy(l_hbm.at[:, at], l.at[:, at], l_sem.at[i]),
            pltpu.make_async_copy(part_hbm.at[at], part.at[at], part_sem.at[i]),
            pltpu.make_async_copy(x_hbm.at[at], x.at[at], x_sem.at[i]),
        )

    def save(i):
        return pltpu.make_async_copy(out.at[block(i)], out_hbm.at[block(i)], out_sem.at[i])

    load_f = pltpu.make_async_copy(f_hbm, f, f_sem)
    load_f.start()
    for i in range(2):
        for copy in loads(i):
            copy.start()
    load_f.wait()

    def step(i, _):
        for copy in loads(i):
            copy.wait()

        @pl.when(i + 2 < STEPS)
        def _():
            for copy in loads(i + 2):
                copy.start()

        at = block(i)
        rows = jnp.concatenate([l[0, at, :], l[1, at, :]], axis=1)
        for n in range(3):
            lo, hi = n * 512, min(n * 512 + 512, LON)
            v = nn(rows, f[:, lo : lo + 512])[:, : hi - lo] + part[at, lo:hi].astype(F32)
            out[at, lo:hi] = (x[at, lo:hi].astype(F32) + half_gelu(v)).astype(BF)
        save(i).start()
        return 0

    lax.fori_loop(0, STEPS, step, 0)
    for i in range(STEPS):
        save(i).wait()


def update(part, l, f, state):
    hbm = pl.BlockSpec(memory_space=pl.ANY)
    dma = pltpu.SemaphoreType.DMA
    whole = pltpu.VMEM((LAT * 16, LON), BF)
    return pl.pallas_call(
        update_kernel,
        out_shape=jax.ShapeDtypeStruct((LAT * 16, LON), BF),
        in_specs=[hbm] * 4,
        out_specs=hbm,
        scratch_shapes=[
            whole,
            pltpu.VMEM(l.shape, BF),
            pltpu.VMEM(f.shape, BF),
            whole,
            whole,
            dma((STEPS,)),
            dma((STEPS,)),
            dma,
            dma((STEPS,)),
            dma((STEPS,)),
        ],
        compiler_params=pltpu.CompilerParams(vmem_limit_bytes=VLIM),
        name="update",
    )(part, l, f, state)


def shards(state_field, slot_order, legendre, degree_gain, mixing):
    state = state_field.transpose(1, 0, 2)
    part, l, f = transform(slot_order, degree_gain, mixing, state, legendre)
    out = update(part, l, f, state.reshape(LAT * 16, LON))
    return out.reshape(LAT, 16, LON).transpose(1, 0, 2)


def solution(mesh):
    placed = (P(("batch", "ord"), "lat", None), P(), P(("lat", "ord"), None, None), P(), P())
    return jax.shard_map(
        shards,
        mesh=mesh,
        in_specs=placed,
        out_specs=P(("batch", "ord"), "lat", None),
        check_vma=False,
    )
```

```python
import functools
import math

import jax
import jax.numpy as jnp
from jax import lax
from jax.experimental import pallas as pl
from jax.experimental.pallas import tpu as pltpu
from jax.sharding import PartitionSpec as P

MESH = pl.DeviceIdType.MESH
BF = jnp.bfloat16
F32 = jnp.float32
LON = 1440
LONP = 1536
NX = 4
NO = 16
ND = NX * NO
MY = 8
PAIRS = 8
LAT = 180
DEG = 720
WIDE = 768
VLIM = 64 * 2**20 - 65536


def nn(a, b):
    return lax.dot_general(a, b, (((1,), (0,)), ((), ())), preferred_element_type=F32)


def nt(a, b):
    return lax.dot_general(a, b, (((1,), (1,)), ((), ())), preferred_element_type=F32)


def one_hot(cond):
    return jnp.where(cond, 1.0, 0.0).astype(BF)


def iota(shape, dim):
    return lax.broadcasted_iota(jnp.int32, shape, dim)


def cos_phase(p):
    p = p - jnp.floor(p * (1.0 / LON)) * LON
    a = (jnp.abs(p - LON / 2) - LON / 4) * (2.0 * math.pi / LON)
    z = a * a
    s = -1.0 / 39916800.0
    for c in (1.0 / 362880.0, -1.0 / 5040.0, 1.0 / 120.0, -1.0 / 6.0):
        s = s * z + c
    return a + a * (z * s)


def shuffle_matrix(transposed):
    i = iota((256, 256), 1 if transposed else 0)
    j = iota((256, 256), 0 if transposed else 1)
    src = (i % 8) * 32 + (i // 16) * 2 + (i // 8) % 2
    return one_hot(src == j)


def greet_signal():
    barrier = pltpu.get_barrier_semaphore()
    me = lax.axis_index("lat") * NO + lax.axis_index("ord")

    def body(k, _):
        d = lax.rem(me + k, ND)
        pl.semaphore_signal(
            barrier,
            inc=1,
            device_id={"lat": d // NO, "ord": lax.rem(d, NO)},
            device_id_type=MESH,
        )
        return 0

    lax.fori_loop(1, ND, body, 0)


def greet_wait():
    pl.semaphore_wait(pltpu.get_barrier_semaphore(), ND - 1)


def partner(k, x, o):
    y, z = o // 4, lax.rem(o, 4)
    dx = lax.rem(x + k // 16, 4)
    dy = lax.rem(y + lax.rem(k // 4, 4), 4)
    dz = lax.rem(z + lax.rem(k, 4), 4)
    return dx, dy * 4 + dz


def send_slot(s, src, dst, send_sem, recv_sem, own_sem):
    x, o = lax.axis_index("lat"), lax.axis_index("ord")
    me = x * NO + o

    def body(k, _):
        dx, do = partner(k, x, o)
        pltpu.make_async_remote_copy(
            src_ref=src.at[s, dx * NO + do],
            dst_ref=dst.at[s, me],
            send_sem=send_sem,
            recv_sem=recv_sem.at[s],
            device_id={"lat": dx, "ord": do},
            device_id_type=MESH,
        ).start()
        return 0

    lax.fori_loop(1, ND, body, 0)
    pltpu.make_async_copy(src.at[s, me], dst.at[s, me], own_sem.at[s]).start()


def wait_slot(s, dst, recv_sem, own_sem):
    me = lax.axis_index("lat") * NO + lax.axis_index("ord")
    pltpu.make_async_copy(dst.at[s, me], dst.at[s, me], own_sem.at[s]).wait()
    others = dst.at[s, 0 : ND - 1]
    pltpu.make_async_copy(others, others, recv_sem.at[s]).wait()


def wait_sent(src, send_sem):
    others = src.at[:, 0 : ND - 1]
    pltpu.make_async_copy(others, others, send_sem).wait()


def lat_select():
    row = iota((DEG, WIDE), 0)
    n = iota((DEG, WIDE), 1)
    tail = n - 512
    main = (n // 128) * LAT + n % 128
    rest = jnp.where(tail % 64 < 52, (tail // 64) * LAT + 128 + tail % 64, -1)
    return one_hot(row == jnp.where(n < 512, main, rest))


def slot_math(got, leg, gain, mix2, out):
    lane = iota((1, 128), 1)
    parts = [got(x) for x in range(NX)]
    rest = [v[:, 256:384].astype(F32) for v in parts]
    turned = [pltpu.roll(v, 64, 1) for v in rest]
    halves = []
    for h in range(2):
        cols = [v[:, h * 128 : h * 128 + 128] for v in parts]
        for x in (0, 2):
            a = rest[x] if h == 0 else turned[x]
            b = turned[x + 1] if h == 0 else rest[x + 1]
            cols.append(jnp.where(lane < 64, a, b).astype(BF))
        spec = nt(jnp.concatenate(cols, axis=1), leg)
        spec = spec.reshape(NO, 2, 8, WIDE) * gain[h * 128 : h * 128 + 128].reshape(NO, 1, 8, WIDE)
        halves.append(spec.reshape(256, WIDE).astype(BF))
    filtered = jnp.concatenate(halves, axis=0)
    syn = []
    for h in range(2):
        mixed = nn(mix2[h * 256 : h * 256 + 256, :], filtered).astype(BF)
        syn.append(nn(mixed, leg))
    for x in range(NX):
        at = 512 + (x // 2) * 128
        a, b = syn[0][:, at : at + 128], syn[1][:, at : at + 128]
        if x % 2:
            a = pltpu.roll(a, 64, 1)
        else:
            b = pltpu.roll(b, 64, 1)
        cols = [v[:, x * 128 : x * 128 + 128] for v in syn] + [jnp.where(lane < 64, a, b)]
        out(x, jnp.concatenate(cols, axis=1).astype(BF))


def swap_matrix():
    i = iota((256, 256), 0)
    j = iota((256, 256), 1)
    return one_hot((i % 16) * 16 + i // 16 == j)


def lat_rows(g, h):
    return h * 128 + g * 16 if g < 8 else 256 + h * 64 + (g - 8) * 16


def table_orders(order_ref):
    d = iota((128, 128), 0) // 2
    m = jnp.zeros((128, 128), jnp.int32)
    for i in range(4):
        m = jnp.where(d // 16 == i, order_ref[i : i + 1, :], m)
    m = jnp.where(iota((128, 128), 1) // 8 == d % 16, m, 0)
    return (m % 256).astype(F32).astype(BF), (m // 256).astype(F32).astype(BF)


def make_table(s, orders, f_ref):
    take = one_hot(iota((128, 128), 0) % 8 == s)
    m = nn(orders[0], take) + 256.0 * nn(orders[1], take)
    r = (iota((128, 1), 0) % 2).astype(F32) * (LON / 4)
    low = m * iota((128, 128), 1).astype(F32) + r
    high = m * (iota((128, 128), 1) * 128).astype(F32)
    root = 1.0 / math.sqrt(LON)
    c0, s0 = cos_phase(low) * root, cos_phase(low + 0.75 * LON) * root
    c1, s1 = cos_phase(high), cos_phase(high + 0.75 * LON)
    lane = iota((1, 128), 1)
    for t in range(LONP // 128):
        v = c0 * c1[:, t : t + 1] - s0 * s1[:, t : t + 1]
        if t == LONP // 128 - 1:
            v = jnp.where(lane < LON - t * 128, v, 0.0)
        f_ref[pl.ds(pl.multiple_of(s * 128, 128), 128), t * 128 : (t + 1) * 128] = v.astype(BF)


DEEP = 4


def load_grid(g, x_hbm, xs, x_sem):
    part = pl.ds(g * 16, min(16, LAT - g * 16))
    return pltpu.make_async_copy(x_hbm.at[part], xs.at[part], x_sem.at[g])


def fill_grid(x_hbm, xs, xb, x_sem, swap):
    for g in range(12):
        load_grid(g, x_hbm, xs, x_sem).wait()
        if g + DEEP < 12:
            load_grid(g + DEEP, x_hbm, xs, x_sem).start()
        v = nn(swap, xs[g * 16 : g * 16 + 16].reshape(256, LON)).astype(BF)
        for c in range(16):
            at = lat_rows(g, c // 8)
            xb[c % 8, at : at + 16, 0:LON] = v[c * 16 : c * 16 + 16]


def forward_slot(s, f_ref, xb, yb, send, shuffle):
    rows = f_ref[pl.ds(pl.multiple_of(s * 128, 128), 128), :]
    for p in range(PAIRS):
        y = nt(rows, xb[p]).astype(BF)
        for q in range(NX):
            yb[q, p * 32 : p * 32 + 32, :] = y[q * 32 : q * 32 + 32, :]
    for q in range(NX):
        v = nn(shuffle, yb[q]).astype(BF)
        send[s, q * 16 : q * 16 + 16] = v.reshape(16, 16, 384)


def split_gain(gain_ref, gp):
    gp[:, DEG:] = jnp.zeros((768, WIDE - DEG), BF)
    t = gain_ref[...].T
    for piece in range(3):
        part = t.astype(BF)
        t = t - part.astype(F32)
        for h in range(2):
            for o in range(NO):
                at = piece * 256 + (h * NO + o) * 8
                gp[at : at + 8, 0:DEG] = part[o * 16 + h * 8 : o * 16 + h * 8 + 8, :]


def slot_gain(m, gp, gs):
    pick = one_hot(iota((WIDE, WIDE), 0) == iota((WIDE, WIDE), 1) + m)
    v = nn(gp[...], pick)
    weight = jnp.where(jnp.full((1, WIDE), m, jnp.int32) == 0, 0.5, 1.0)
    gs[...] = (v[0:256] + v[256:512] + v[512:768]) * weight


def two_part_mixing(mix_ref, mix2):
    i = iota((512, 256), 0)
    c = (i // 16) % NO * 16 + (i // 256) * 8 + i % 8
    j = iota((512, 256), 1)
    acc = jnp.zeros((512, 512), F32)
    for r in range(2):
        e = one_hot(c + 256 * ((i // 8) % 2) == j + 256 * r)
        half = nt(e, mix_ref[...]).astype(BF)
        acc = acc + nt(half, e)
    mix2[...] = acc.astype(BF)


def collect(s, ret, bb, tb, lb, shuffle_back, swap):
    for x in range(NX):
        v = nn(shuffle_back, ret[s, x * 16 : x * 16 + 16].reshape(256, 384)).astype(BF)
        for p in range(PAIRS):
            bb[p, x * 32 : x * 32 + 32, :] = v[p * 32 : p * 32 + 32, :]

    for p in range(PAIRS):
        t = bb[p].T
        for h in range(2):
            for g in range(12):
                at = lat_rows(g, h)
                tb[g, h * 128 + p * 16 : h * 128 + p * 16 + 16, :] = t[at : at + 16]

    for g in range(12):
        lb[g * 256 : g * 256 + 256, :] = nn(swap, tb[g]).astype(BF)


LAST = MY - 2
BLOCK = 288
BLOCKS = LAT * 16 // BLOCK


def gelu_of_half(h):
    k = 2.0 * math.sqrt(2.0 / math.pi)
    return h + h * jnp.tanh(h * (k + (k * 4.0 * 0.044715) * (h * h)))


def transform_kernel(
    so_ref, order_ref, gain_hbm, mix_hbm, x_hbm, leg_hbm,
    part_hbm, l_hbm, f_hbm,
    gain, mix, fb, send, got, ans, ret, leg, legp, select, gp, gs, mix2, bb, tb, lb,
    gain_sem, mix_sem, x_sem, leg_sem, out_sem, l_sem, f_sem,
    send_sem, recv_sem, own_sem, send2_sem, recv2_sem, own2_sem,
):
    me = lax.axis_index("lat") * NO + lax.axis_index("ord")
    swap = swap_matrix()
    load_gain = pltpu.make_async_copy(gain_hbm, gain, gain_sem)
    load_mix = pltpu.make_async_copy(mix_hbm, mix, mix_sem)

    def load_leg(s):
        return pltpu.make_async_copy(leg_hbm.at[s], leg.at[lax.rem(s, 2)], leg_sem.at[lax.rem(s, 2)])

    def first(xs, xb, yb):
        for g in range(DEEP):
            load_grid(g, x_hbm, xs, x_sem).start()
        greet_signal()
        load_gain.start()
        load_mix.start()
        load_leg(0).start()
        load_leg(1).start()
        orders = table_orders(order_ref)
        shuffle = shuffle_matrix(False)
        xs[LAT:192] = jnp.zeros((192 - LAT, 16, LON), BF)
        xb[:, :, LON:] = jnp.zeros((PAIRS, 384, LONP - LON), BF)
        make_table(0, orders, fb)
        fill_grid(x_hbm, xs, xb, x_sem, swap)
        greet_wait()

        def slot(s, _):
            forward_slot(s, fb, xb, yb, send, shuffle)
            send_slot(s, send, got, send_sem, recv_sem, own_sem)

            @pl.when(s + 1 < MY)
            def _():
                make_table(s + 1, orders, fb)

            return 0

        lax.fori_loop(0, MY, slot, 0)

    pl.run_scoped(
        first,
        pltpu.VMEM((192, 16, LON), BF),
        pltpu.VMEM((PAIRS, 384, LONP), BF),
        pltpu.VMEM((NX, 256, 384), BF),
    )

    load_mix.wait()
    two_part_mixing(mix, mix2)
    load_gain.wait()
    split_gain(gain, gp)
    select[...] = lat_select()
    legp[DEG:WIDE, :] = jnp.zeros((WIDE - DEG, WIDE), BF)

    def slot(s, _):
        slot_gain(so_ref[me * MY + s], gp, gs)
        load_leg(s).wait()
        legp[0:DEG, :] = nn(leg[lax.rem(s, 2)], select[...]).astype(BF)

        @pl.when(s + 2 < MY)
        def _():
            load_leg(s + 2).start()

        wait_slot(s, got, recv_sem, own_sem)

        def out(x, v):
            ans[s, x * 16 : x * 16 + 16] = v.reshape(16, 16, 384)

        slot_math(
            lambda x: got[s, x * 16 : x * 16 + 16].reshape(256, 384), legp[...], gs[...], mix2, out
        )
        send_slot(s, ans, ret, send2_sem, recv2_sem, own2_sem)
        return 0

    lax.fori_loop(0, MY, slot, 0)

    save_f = pltpu.make_async_copy(fb.at[LAST * 128 :], f_hbm, f_sem)
    save_f.start()

    def last(acc, out):
        shuffle_back = shuffle_matrix(True)

        def block(i):
            return pl.ds(pl.multiple_of(i * BLOCK, 32), BLOCK)

        def save(i):
            at = lax.rem(i, 2)
            return pltpu.make_async_copy(out.at[at], part_hbm.at[block(i)], out_sem.at[at])

        def gather(s, k):
            wait_slot(s, ret, recv2_sem, own2_sem)
            collect(s, ret, bb, tb, lb.at[k], shuffle_back, swap)

        def product(t, i, n):
            v = jnp.concatenate([lb[0, block(i), :], lb[1, block(i), :]], axis=1)
            rows = pl.ds(pl.multiple_of(t * 256, 256), 256)
            return nn(v, fb[rows, n * 512 : n * 512 + 512])

        def add(t, start):
            def body(i, _):
                for n in range(3):
                    lanes = slice(n * 512, n * 512 + 512)
                    v = product(t, i, n)
                    acc[block(i), lanes] = v if start else acc[block(i), lanes] + v
                return 0

            lax.fori_loop(0, BLOCKS, body, 0)

        def finish(i, _):
            @pl.when(i >= 2)
            def _():
                save(i - 2).wait()

            for n in range(3):
                lo, hi = n * 512, min(n * 512 + 512, LON)
                v = acc[block(i), lo : lo + 512] + product(LAST // 2 - 1, i, n)
                out[lax.rem(i, 2), :, lo:hi] = v[:, : hi - lo].astype(BF)
            save(i).start()
            return 0

        for t in range(LAST // 2):
            gather(2 * t, 0)
            gather(2 * t + 1, 1)
            if t < LAST // 2 - 1:
                add(t, t == 0)
        lax.fori_loop(0, BLOCKS, finish, 0)
        for k in range(2):
            gather(LAST + k, k)
            save_l(k).start()
        save(BLOCKS - 2).wait()
        save(BLOCKS - 1).wait()

    def save_l(k):
        return pltpu.make_async_copy(lb.at[k, 0 : LAT * 16], l_hbm.at[k], l_sem.at[k])

    pl.run_scoped(
        last,
        pltpu.VMEM((LAT * 16, LONP), F32),
        pltpu.VMEM((2, BLOCK, LON), BF),
    )
    save_f.wait()
    save_l(0).wait()
    save_l(1).wait()
    wait_sent(send, send_sem)
    wait_sent(ans, send2_sem)


def transform(slot_order, degree_gain, mixing, state, legendre):
    vm = pl.BlockSpec(memory_space=pltpu.VMEM)
    hbm = pl.BlockSpec(memory_space=pl.ANY)
    dma = pltpu.SemaphoreType.DMA
    message = pltpu.VMEM((MY, ND, 16, 384), BF)
    return pl.pallas_call(
        transform_kernel,
        out_shape=(
            jax.ShapeDtypeStruct((LAT * 16, LON), BF),
            jax.ShapeDtypeStruct((2, LAT * 16, 128), BF),
            jax.ShapeDtypeStruct((256, LONP), BF),
        ),
        in_specs=[pl.BlockSpec(memory_space=pltpu.SMEM), vm, hbm, hbm, hbm, hbm],
        out_specs=(hbm, hbm, hbm),
        scratch_shapes=[
            pltpu.VMEM((DEG, 256), F32),
            pltpu.VMEM((256, 256), BF),
            pltpu.VMEM((2 * MY * ND, LONP), BF),
            message,
            message,
            message,
            message,
            pltpu.VMEM((2, DEG, DEG), BF),
            pltpu.VMEM((WIDE, WIDE), BF),
            pltpu.VMEM((DEG, WIDE), BF),
            pltpu.VMEM((768, WIDE), BF),
            pltpu.VMEM((256, WIDE), F32),
            pltpu.VMEM((512, 512), BF),
            pltpu.VMEM((PAIRS, 128, 384), BF),
            pltpu.VMEM((12, 256, 128), BF),
            pltpu.VMEM((2, 3072, 128), BF),
            dma,
            dma,
            dma((12,)),
            dma((2,)),
            dma((2,)),
            dma((2,)),
            dma,
            dma,
            dma((MY,)),
            dma((MY,)),
            dma,
            dma((MY,)),
            dma((MY,)),
        ],
        compiler_params=pltpu.CompilerParams(
            collective_id=0, has_side_effects=True, vmem_limit_bytes=VLIM
        ),
        name="transform",
    )(
        slot_order, slot_order.reshape(4, 128), degree_gain, mixing, state, legendre,
    )


ROWS = 480
STEPS = LAT * 16 // ROWS


def update_kernel(
    part_hbm, l_hbm, f_hbm, x_hbm, out_hbm,
    part, l, f, x, out, part_sem, l_sem, f_sem, x_sem, out_sem,
):
    def block(i):
        return pl.ds(pl.multiple_of(i * ROWS, 32), ROWS)

    def loads(i):
        at = block(i)
        return (
            pltpu.make_async_copy(l_hbm.at[:, at], l.at[:, at], l_sem.at[i]),
            pltpu.make_async_copy(part_hbm.at[at], part.at[at], part_sem.at[i]),
            pltpu.make_async_copy(x_hbm.at[at], x.at[at], x_sem.at[i]),
        )

    def save(i):
        return pltpu.make_async_copy(out.at[block(i)], out_hbm.at[block(i)], out_sem.at[i])

    load_f = pltpu.make_async_copy(f_hbm, f, f_sem)
    load_f.start()
    for i in range(2):
        for copy in loads(i):
            copy.start()
    load_f.wait()

    def step(i, _):
        for copy in loads(i):
            copy.wait()

        @pl.when(i + 2 < STEPS)
        def _():
            for copy in loads(i + 2):
                copy.start()

        at = block(i)
        rows = jnp.concatenate([l[0, at, :], l[1, at, :]], axis=1)
        for n in range(3):
            lo, hi = n * 512, min(n * 512 + 512, LON)
            v = nn(rows, f[:, lo : lo + 512])[:, : hi - lo] + part[at, lo:hi].astype(F32)
            out[at, lo:hi] = (x[at, lo:hi].astype(F32) + gelu_of_half(v)).astype(BF)
        save(i).start()
        return 0

    lax.fori_loop(0, STEPS, step, 0)
    for i in range(STEPS):
        save(i).wait()


def update(part, l, f, state):
    hbm = pl.BlockSpec(memory_space=pl.ANY)
    dma = pltpu.SemaphoreType.DMA
    whole = pltpu.VMEM((LAT * 16, LON), BF)
    return pl.pallas_call(
        update_kernel,
        out_shape=jax.ShapeDtypeStruct((LAT * 16, LON), BF),
        in_specs=[hbm] * 4,
        out_specs=hbm,
        scratch_shapes=[
            whole,
            pltpu.VMEM(l.shape, BF),
            pltpu.VMEM(f.shape, BF),
            whole,
            whole,
            dma((STEPS,)),
            dma((STEPS,)),
            dma,
            dma((STEPS,)),
            dma((STEPS,)),
        ],
        compiler_params=pltpu.CompilerParams(vmem_limit_bytes=VLIM),
        name="update",
    )(part, l, f, state)


def shards(state_field, slot_order, legendre, degree_gain, mixing):
    state = state_field.transpose(1, 0, 2)
    part, l, f = transform(slot_order, degree_gain, mixing, state, legendre)
    out = update(part, l, f, state.reshape(LAT * 16, LON))
    return out.reshape(LAT, 16, LON).transpose(1, 0, 2)


def solution(mesh):
    placed = (P(("batch", "ord"), "lat", None), P(), P(("lat", "ord"), None, None), P(), P())
    return jax.shard_map(
        shards,
        mesh=mesh,
        in_specs=placed,
        out_specs=P(("batch", "ord"), "lat", None),
        check_vma=False,
    )
```
